8 devices in a mesh: dp: 1 (over z), pp: 2 (over y), tp: 4 (over x, core).
Axes of the slice: x: 2, y: 2, z: 1, core: 2. Of those that a mesh axis runs over, the one named last changes fastest.
Arguments:
- x_in: bfloat16 [8, 512, 6144], P('dp')
- seq_len: int32 [8], P('dp')
- norm_attn: bfloat16 [2, 6144], P('pp')
- w_qa: bfloat16 [2, 6144, 1536], P('pp')
- norm_q: bfloat16 [2, 1536], P('pp')
- w_qb: bfloat16 [2, 1536, 12288], P('pp', None, 'tp')
- w_kva: bfloat16 [2, 6144, 576], P('pp')
- norm_kv: bfloat16 [2, 512], P('pp')
- w_kvb: bfloat16 [2, 512, 16384], P('pp', None, 'tp')
- w_o: bfloat16 [2, 8192, 6144], P('pp', 'tp')
- norm_mlp: bfloat16 [2, 6144], P('pp')
- w_gate: bfloat16 [2, 6144, 12288], P('pp', None, 'tp')
- w_up: bfloat16 [2, 6144, 12288], P('pp', None, 'tp')
- w_down: bfloat16 [2, 12288, 6144], P('pp', 'tp')
- norm_final: bfloat16 [6144], replicated
Outputs:
- output 1: bfloat16 [2, 8, 512, 512], P('pp', 'dp')
- output 2: bfloat16 [2, 8, 512, 64], P('pp', 'dp')
- output 3: bfloat16 [8, 6144], P('dp')
All inputs are finite; a program needn't handle non-finite values.
Results may differ from the reference program's by a relative error of at most 0.0180411.
Values are sent between devices in bfloat16 or wider.
A program may use at most 1 GiB of HBM per device.

```python
import math
import jax
import jax.numpy as jnp
from jax import lax

D_MODEL = 6144
HEADS = 64
Q_LORA = 1536
KV_LORA = 512
QK_NOPE = 128
QK_ROPE = 64
V_HEAD = 128
FFN_DIM = 12288
SEQ_LEN = 512
BATCH = 8
LAYERS = 2
RMS_EPS = 1e-5
ROPE_BASE = 10000.0
SCALE_DEPTH = 1.4


def draw_weight(key, shape, fan_in):
    return (jax.random.normal(key, shape, jnp.float32) * fan_in ** -0.5).astype(jnp.bfloat16)


def draw_gain(key, shape):
    return (1.0 + 0.3 * jax.random.normal(key, shape, jnp.float32)).astype(jnp.bfloat16)


def setup_inputs(seed: int = 0, part: int = 0) -> dict:
    base_key = jax.random.key(seed)
    part_key = jax.random.fold_in(base_key, part)
    act_key, len_key = jax.random.split(part_key)
    weight_keys = jax.random.split(base_key, 13)
    slot_ids = jnp.arange(BATCH)
    drawn = jax.random.randint(len_key, (BATCH,), 1, SEQ_LEN + 1)
    seq_len = jnp.where(slot_ids == 0, SEQ_LEN, jnp.where(slot_ids == BATCH - 1, 1, drawn)).astype(jnp.int32)
    return {
        "x_in": jax.random.normal(act_key, (BATCH, SEQ_LEN, D_MODEL), jnp.float32).astype(jnp.bfloat16),
        "seq_len": seq_len,
        "norm_attn": draw_gain(weight_keys[0], (LAYERS, D_MODEL)),
        "w_qa": draw_weight(weight_keys[1], (LAYERS, D_MODEL, Q_LORA), D_MODEL),
        "norm_q": draw_gain(weight_keys[2], (LAYERS, Q_LORA)),
        "w_qb": draw_weight(weight_keys[3], (LAYERS, Q_LORA, HEADS * (QK_NOPE + QK_ROPE)), Q_LORA),
        "w_kva": draw_weight(weight_keys[4], (LAYERS, D_MODEL, KV_LORA + QK_ROPE), D_MODEL),
        "norm_kv": draw_gain(weight_keys[5], (LAYERS, KV_LORA)),
        "w_kvb": draw_weight(weight_keys[6], (LAYERS, KV_LORA, HEADS * (QK_NOPE + V_HEAD)), KV_LORA),
        "w_o": draw_weight(weight_keys[7], (LAYERS, HEADS * V_HEAD, D_MODEL), HEADS * V_HEAD),
        "norm_mlp": draw_gain(weight_keys[8], (LAYERS, D_MODEL)),
        "w_gate": draw_weight(weight_keys[9], (LAYERS, D_MODEL, FFN_DIM), D_MODEL),
        "w_up": draw_weight(weight_keys[10], (LAYERS, D_MODEL, FFN_DIM), D_MODEL),
        "w_down": draw_weight(weight_keys[11], (LAYERS, FFN_DIM, D_MODEL), FFN_DIM),
        "norm_final": draw_gain(weight_keys[12], (D_MODEL,)),
    }


def rms_norm(values_in, gain):
    wide_vals = values_in.astype(jnp.float32)
    inv_rms = lax.rsqrt(jnp.mean(wide_vals * wide_vals, axis=-1, keepdims=True) + RMS_EPS)
    return (wide_vals * inv_rms * gain.astype(jnp.float32)).astype(jnp.bfloat16)


def apply_rope(values_in, cos_t, sin_t):
    half_dim = values_in.shape[-1] // 2
    wide_vals = values_in.astype(jnp.float32)
    lo_half = wide_vals[..., :half_dim]
    hi_half = wide_vals[..., half_dim:]
    return jnp.concatenate([lo_half * cos_t - hi_half * sin_t, hi_half * cos_t + lo_half * sin_t], axis=-1).astype(jnp.bfloat16)


def matmul_wide(act_in, weight):
    flat_act = act_in.reshape(-1, act_in.shape[-1])
    return jnp.dot(flat_act, weight, preferred_element_type=jnp.float32).reshape(act_in.shape[:-1] + (weight.shape[-1],))


def reference(x_in, seq_len, norm_attn, w_qa, norm_q, w_qb, w_kva, norm_kv, w_kvb, w_o, norm_mlp, w_gate, w_up, w_down, norm_final):
    res_scale = SCALE_DEPTH / math.sqrt(LAYERS)
    half_dim = QK_ROPE // 2
    inv_freq = ROPE_BASE ** (-2.0 * jnp.arange(half_dim, dtype=jnp.float32) / QK_ROPE)
    angle = jnp.arange(SEQ_LEN, dtype=jnp.float32)[:, None] * inv_freq[None, :]
    cos_t = jnp.cos(angle)
    sin_t = jnp.sin(angle)
    positions = jnp.arange(SEQ_LEN)
    causal = positions[:, None] >= positions[None, :]
    key_ok = positions[None, :] < seq_len[:, None]
    score_scale = (QK_NOPE + QK_ROPE) ** -0.5

    def row_attention(row):
        q_nope, q_rope, k_nope, k_rope, values, row_ok = row
        scores = (jnp.einsum("shd,thd->hst", q_nope.astype(jnp.float32), k_nope.astype(jnp.float32))
                  + jnp.einsum("shd,td->hst", q_rope.astype(jnp.float32), k_rope.astype(jnp.float32))) * score_scale
        allowed = causal & row_ok[None, :]
        scores = jnp.where(allowed[None], scores, -1e30)
        attn_probs = jax.nn.softmax(scores, axis=-1).astype(jnp.bfloat16)
        return jnp.einsum("hst,thd->shd", attn_probs.astype(jnp.float32), values.astype(jnp.float32)).astype(jnp.bfloat16)

    def layer(hidden, weights):
        g_attn, wq_down, g_q, wq_up, wkv_down, g_kv, wkv_up, wo_layer, g_mlp, wgate_layer, wup_layer, wdown_layer = weights
        normed = rms_norm(hidden, g_attn)
        q_down = rms_norm(matmul_wide(normed, wq_down).astype(jnp.bfloat16), g_q)
        latent_raw = matmul_wide(normed, wkv_down).astype(jnp.bfloat16)
        c_kv = rms_norm(latent_raw[..., :KV_LORA], g_kv)
        k_rope = apply_rope(latent_raw[..., KV_LORA:], cos_t, sin_t)
        q_full = matmul_wide(q_down, wq_up).astype(jnp.bfloat16).reshape(BATCH, SEQ_LEN, HEADS, QK_NOPE + QK_ROPE)
        kv_full = matmul_wide(c_kv, wkv_up).astype(jnp.bfloat16).reshape(BATCH, SEQ_LEN, HEADS, QK_NOPE + V_HEAD)
        q_rope = apply_rope(q_full[..., QK_NOPE:], cos_t[:, None, :], sin_t[:, None, :])
        attn_out = lax.map(row_attention, (q_full[..., :QK_NOPE], q_rope, kv_full[..., :QK_NOPE], k_rope, kv_full[..., QK_NOPE:], key_ok))
        attn_proj = matmul_wide(attn_out.reshape(BATCH, SEQ_LEN, HEADS * V_HEAD), wo_layer).astype(jnp.bfloat16)
        hidden = (hidden.astype(jnp.float32) + res_scale * attn_proj.astype(jnp.float32)).astype(jnp.bfloat16)
        normed = rms_norm(hidden, g_mlp)
        hidden_act = (jax.nn.silu(matmul_wide(normed, wgate_layer)) * matmul_wide(normed, wup_layer)).astype(jnp.bfloat16)
        mlp_proj = matmul_wide(hidden_act, wdown_layer).astype(jnp.bfloat16)
        hidden = (hidden.astype(jnp.float32) + res_scale * mlp_proj.astype(jnp.float32)).astype(jnp.bfloat16)
        return hidden, (c_kv, k_rope)

    hidden, caches = lax.scan(layer, x_in, (norm_attn, w_qa, norm_q, w_qb, w_kva, norm_kv, w_kvb, w_o, norm_mlp, w_gate, w_up, w_down))
    last_tok = jnp.take_along_axis(hidden, (seq_len - 1)[:, None, None], axis=1)[:, 0]
    return caches[0], caches[1], rms_norm(last_tok, norm_final)
```

```python
import functools
import math
import jax
import jax.numpy as jnp
from jax import lax
from jax.experimental import pallas as pl
from jax.experimental.pallas import tpu as pltpu
from jax.sharding import Mesh, PartitionSpec as P

RMS_EPS = 1e-5
ROPE_BASE = 10000.0
SCALE_DEPTH = 1.4
BF16, F32 = jnp.bfloat16, jnp.float32
ROWS = 128
HEAD_BLOCK = 4
OUT_COLS = 768
ACT_COLS = 256
DOWN_COLS = 256
VMEM_LIMIT = 60 * 2 ** 20


def dot(lhs, rhs):
    return jnp.dot(lhs, rhs, preferred_element_type=F32)


def dot_t(lhs, rhs):
    return lax.dot_general(lhs, rhs, (((1,), (1,)), ((), ())), preferred_element_type=F32)


def rms_wide(wide, gain):
    inv = lax.rsqrt(jnp.mean(wide * wide, axis=-1, keepdims=True) + RMS_EPS)
    return (wide * inv * gain).astype(BF16)


def rms_rows(x_ref, rows, count, gain_ref, out_ref):
    width, cols = x_ref.shape[1], 256
    squares = jnp.zeros((count, cols), F32)
    for first in range(0, width, cols):
        wide = x_ref[rows, first:first + cols].astype(F32)
        squares = squares + wide * wide
    inv = lax.rsqrt(jnp.sum(squares, axis=-1, keepdims=True) * (1.0 / width) + RMS_EPS)
    for first in range(0, width, cols):
        wide = x_ref[rows, first:first + cols].astype(F32)
        out_ref[rows, first:first + cols] = (wide * inv * gain_ref[:, first:first + cols].astype(F32)).astype(BF16)


def rms_norm(values_in, gain):
    return rms_wide(values_in.astype(F32), gain.astype(F32))


def rope_tables(seq, rope):
    inv_freq = ROPE_BASE ** (-2.0 * jnp.arange(rope // 2, dtype=F32) / rope)
    angle = jnp.arange(seq, dtype=F32)[:, None] * inv_freq[None, :]
    cos_t, sin_t = jnp.cos(angle), jnp.sin(angle)
    return jnp.concatenate([cos_t, cos_t], axis=-1), jnp.concatenate([-sin_t, sin_t], axis=-1)


def apply_rope(values_in, cos_t, sin_t):
    half = values_in.shape[-1] // 2
    wide = values_in.astype(F32)
    swapped = jnp.concatenate([wide[..., half:], wide[..., :half]], axis=-1)
    return (wide * cos_t + swapped * sin_t).astype(BF16)


def call(kernel, grid, scalars, inputs, outputs, scratch, flops, moved):
    return pl.pallas_call(
        kernel,
        grid_spec=pltpu.PrefetchScalarGridSpec(
            num_scalar_prefetch=1, grid=grid,
            in_specs=[spec for _, spec in inputs], out_specs=[spec for _, spec in outputs], scratch_shapes=scratch),
        out_shape=[jax.ShapeDtypeStruct(shape, dtype) for (shape, dtype), _ in outputs],
        compiler_params=pltpu.CompilerParams(dimension_semantics=("arbitrary",) * len(grid), vmem_limit_bytes=VMEM_LIMIT),
        cost_estimate=pl.CostEstimate(flops=int(flops), transcendentals=0, bytes_accessed=int(moved)),
    )(scalars, *[array for array, _ in inputs])


ANY = pl.BlockSpec(memory_space=pl.ANY)
TOKEN = ((8, 128), F32)


def fixed(*shape):
    return pl.BlockSpec(shape, lambda *_: (0,) * len(shape))


ORDER = [
    ("down", 0), ("att", 0), ("down", 1), ("suma", 0), ("att", 1), ("down", 2),
    ("suma", 1), ("res", 0), ("att", 2), ("down", 3), ("res", 1), ("att", 3),
    ("suma", 2), ("mlp", 0), ("res", 2), ("suma", 3), ("mlp", 1), ("summ", 0),
    ("res", 3), ("summ", 1), ("mlp", 2), ("next", 0), ("summ", 2), ("mlp", 3),
    ("next", 1), ("summ", 3), ("next", 2), ("next", 3),
]


def down_kernel(dims, info, x_ref, g_attn, wq_ref, g_q, wkv_hbm, g_kv, cos_ref, sin_ref, _, joined_ref, token_ref,
                u_ref, raw_ref, wkv_ref, sem):
    q_rank, kv_rank, rope, steps = dims
    step = pl.program_id(0)
    active = info[0] == 1
    copy = pltpu.make_async_copy(wkv_hbm, wkv_ref, sem)
    seq = x_ref.shape[0]

    @pl.when((step == 0) & active)
    def _():
        copy.start()
        for first in range(0, seq, ROWS):
            for inner in range(first, first + ROWS, 32):
                rms_rows(x_ref, pl.ds(inner, 32), 32, g_attn, u_ref)
            rows = pl.ds(first, ROWS)
            raw_ref[rows, :DOWN_COLS] = dot(u_ref[rows, :], wq_ref[...]).astype(BF16)

    @pl.when((step > 0) & (step < steps) & active)
    def _():
        cols = pl.ds(pl.multiple_of(step * DOWN_COLS, DOWN_COLS), DOWN_COLS)
        raw_ref[:, cols] = dot(u_ref[...], wq_ref[...]).astype(BF16)

    @pl.when((step == steps) & active)
    def _():
        copy.wait()
        low = dot_t(u_ref[...], wkv_ref[...]).astype(BF16)
        for first in range(0, seq, 32):
            rows = pl.ds(first, 32)
            joined_ref[rows, :q_rank] = rms_norm(raw_ref[rows, :], g_q[...])
            joined_ref[rows, q_rank:q_rank + kv_rank] = rms_norm(low[first:first + 32, :kv_rank], g_kv[...])
            joined_ref[rows, q_rank + kv_rank:] = jnp.concatenate(
                [apply_rope(low[first:first + 32, kv_rank:], cos_ref[rows, :], sin_ref[rows, :]), jnp.zeros((32, rope), BF16)], axis=-1)

    @pl.when(step == steps)
    def _():
        token_ref[...] = jnp.zeros_like(token_ref)


def attention_kernel(dims, info, own_hbm, other_hbm, wq_ref, wkv_ref, wo_ref, cos_ref, sin_ref, _, near_ref, far_ref, token_ref,
                     joined, outs, sems):
    q_rank, kv_rank, nope, rope, v_head, steps = dims
    step = pl.program_id(0)
    active = info[0] == 1
    qk, seq = nope + rope, joined.shape[1]
    copies = [pltpu.make_async_copy(ref, joined.at[i], sems.at[i]) for i, ref in enumerate((own_hbm, other_hbm))]

    @pl.when((step == 0) & active)
    def _():
        copies[0].start()
        copies[1].start()
        copies[0].wait()

    @pl.when((step == 1) & active)
    def _():
        copies[1].wait()

    @pl.when((step < steps) & active)
    def _():
        prompt = step % 2
        length = info[2 + prompt]
        chip = info[1]
        q_all = dot(joined[prompt, :, :q_rank], wq_ref[...]).astype(BF16)
        kv_all = dot(joined[prompt, :, q_rank:q_rank + kv_rank], wkv_ref[...]).astype(BF16)
        k_rope = joined[prompt, :, q_rank + kv_rank:q_rank + kv_rank + rope]
        cos_t, sin_t = cos_ref[...], sin_ref[...]
        for head in range(HEAD_BLOCK):
            q_rope = apply_rope(q_all[:, head * qk + nope:(head + 1) * qk], cos_t, sin_t)
            queries = jnp.concatenate([q_all[:, head * qk:head * qk + nope], q_rope], axis=-1)
            base = head * (nope + v_head)
            keys = jnp.concatenate([kv_all[:, base:base + nope], k_rope], axis=-1)
            values = kv_all[:, base + nope:base + nope + v_head]
            cols = pl.ds(pl.multiple_of(((step // 2) * HEAD_BLOCK + head) * v_head, v_head), v_head)
            for first in range(0, seq, ROWS):
                ends = first + ROWS
                scores = lax.dot_general(queries[first:ends], keys[:ends], (((1,), (1,)), ((), ())),
                                         preferred_element_type=F32) * (qk ** -0.5 * math.log2(math.e))
                limit = jnp.minimum(lax.broadcasted_iota(jnp.int32, (ROWS, 1), 0) + first, length - 1)
                scores = jnp.where(lax.broadcasted_iota(jnp.int32, (ROWS, ends), 1) <= limit, scores, -1e30)
                grown = jnp.exp2(scores - jnp.max(scores, axis=-1, keepdims=True))
                probs = (grown * (1.0 / jnp.sum(grown, axis=-1, keepdims=True))).astype(BF16)
                half = seq // 2
                place = jnp.bitwise_xor(first // half, chip) * half + first % half
                outs[prompt, pl.ds(pl.multiple_of(place, ROWS), ROWS), cols] = dot(probs, values[:ends]).astype(BF16)

    @pl.when((step >= steps) & active)
    def _():
        for prompt, out_ref in enumerate((near_ref, far_ref)):
            for first in range(0, seq, 256):
                out_ref[pl.ds(first, 256), :] = dot(outs[prompt, pl.ds(first, 256), :], wo_ref[...]).astype(BF16)

    @pl.when(step == pl.num_programs(0) - 1)
    def _():
        token_ref[...] = jnp.zeros_like(token_ref)


def mlp_kernel(steps, info, m0, m1, m2, m3, w1_ref, w3_ref, w2_ref, _, near_ref, far_ref, token_ref, rows_ref, act_ref, sems):
    step = pl.program_id(0)
    active = info[0] == 1
    piece = m0.shape[0]
    copies = [pltpu.make_async_copy(ref, rows_ref.at[pl.ds(i * piece, piece)], sems.at[i]) for i, ref in enumerate((m0, m1, m2, m3))]

    def gate(first_step):
        cols = pl.ds(pl.multiple_of(step * ACT_COLS, ACT_COLS), ACT_COLS)
        for i in range(4):
            if first_step:
                copies[i].wait()
            rows = pl.ds(i * piece, piece)
            wide = dot(rows_ref[rows, :], w1_ref[...])
            act_ref[rows, cols] = (wide * jax.nn.sigmoid(wide) * dot(rows_ref[rows, :], w3_ref[...])).astype(BF16)

    @pl.when((step == 0) & active)
    def _():
        for copy in copies:
            copy.start()
        gate(True)

    @pl.when((step > 0) & (step < steps) & active)
    def _():
        gate(False)

    @pl.when((step >= steps) & active)
    def _():
        for i in range(4):
            out_ref = near_ref if i < 2 else far_ref
            out_ref[pl.ds((i % 2) * piece, piece), :] = dot(act_ref[pl.ds(i * piece, piece), :], w2_ref[...]).astype(BF16)

    @pl.when(step == pl.num_programs(0) - 1)
    def _():
        token_ref[...] = jnp.zeros_like(token_ref)


def add_kernel(info, a_ref, b_ref, _, out_ref, token_ref):
    out_ref[...] = (a_ref[...].astype(F32) + b_ref[...].astype(F32)).astype(BF16)
    token_ref[...] = jnp.zeros_like(token_ref)


def join(scale, hidden, near, other_core, other_chip):
    both = (near.astype(F32) + other_core.astype(F32)).astype(BF16)
    branch = (both.astype(F32) + other_chip.astype(F32)).astype(BF16)
    return (hidden.astype(F32) + scale * branch.astype(F32)).astype(BF16)


def residual_kernel(scale, info, x_ref, near_ref, core_ref, chip_ref, gain, _, h_ref, m_ref, token_ref):
    hidden = join(scale, x_ref[...], near_ref[...], core_ref[...], chip_ref[...])
    h_ref[...] = hidden
    m_ref[...] = rms_norm(hidden, gain[...])
    token_ref[...] = jnp.zeros_like(token_ref)


def next_kernel(scale, kv_rank, info, h_ref, near_ref, core_ref, chip_ref, g_attn, wkv_ref, g_kv, cos_ref, sin_ref, _,
                msg_ref, token_ref, row_ref):
    step = pl.program_id(0)
    rows = h_ref.shape[0]
    total = rows * pl.num_programs(0)
    hidden = join(scale, h_ref[...], near_ref[...], core_ref[...], chip_ref[...])
    low = dot_t(rms_norm(hidden, g_attn[...]), wkv_ref[...]).astype(BF16)
    msg_ref[pl.ds(pl.multiple_of(step * rows, rows), rows), :kv_rank] = rms_norm(low[:, :kv_rank], g_kv[...])
    turned = apply_rope(low[:, kv_rank:], cos_ref[...], sin_ref[...])
    msg_ref[pl.ds(pl.multiple_of(step * rows, rows), rows), kv_rank:] = jnp.concatenate([turned, jnp.zeros_like(turned)], axis=-1)
    wanted = info[2] - 1 - info[1] * total - step * rows
    picked = jnp.where(lax.broadcasted_iota(jnp.int32, (rows, 1), 0) == wanted, hidden.astype(F32), 0.0)
    picked = jnp.sum(picked, axis=0, keepdims=True)

    @pl.when(step == 0)
    def _():
        row_ref[...] = jnp.broadcast_to(picked, row_ref.shape)

    @pl.when(step > 0)
    def _():
        row_ref[...] += jnp.broadcast_to(picked, row_ref.shape)

    @pl.when(step == pl.num_programs(0) - 1)
    def _():
        width = msg_ref.shape[1]
        depth = row_ref.shape[1]
        parts = []
        for first in range(0, depth, width):
            part = row_ref[0:1, first:min(first + width, depth)]
            if part.shape[1] < width:
                part = jnp.concatenate([part, jnp.zeros((1, width - part.shape[1]), F32)], axis=-1)
            parts.append(part)
        parts.append(jnp.zeros((16 - len(parts), width), F32))
        msg_ref[pl.ds(total, 16), :] = jnp.concatenate(parts, axis=0).astype(BF16)

    token_ref[...] = jnp.zeros_like(token_ref)


def last_kernel(dims, info, q_ref, c_ref, wkv_ref, out_ref):
    kv_rank, nope, rope, v_head = dims
    for prompt in range(2):
        length = info[2 + prompt]
        kv_all = dot(c_ref[prompt, :, :kv_rank], wkv_ref[...]).astype(BF16)
        k_rope = c_ref[prompt, :, kv_rank:kv_rank + rope]
        for head in range(HEAD_BLOCK):
            base = head * (nope + v_head)
            keys = jnp.concatenate([kv_all[:, base:base + nope], k_rope], axis=-1)
            query = q_ref[prompt, head]
            scores = lax.dot_general(query, keys, (((1,), (1,)), ((), ())), preferred_element_type=F32) * (nope + rope) ** -0.5
            scores = jnp.where(lax.broadcasted_iota(jnp.int32, scores.shape, 1) < length, scores, -1e30)
            grown = jnp.exp(scores - jnp.max(scores, axis=-1, keepdims=True))
            probs = (grown * (1.0 / jnp.sum(grown, axis=-1, keepdims=True))).astype(BF16)
            out_ref[prompt, :, head * v_head:(head + 1) * v_head] = dot(probs, kv_all[:, base + nope:base + nope + v_head]).astype(BF16)


def rows_kernel(info, rows_ref, w_ref, out_ref):
    out_ref[...] = dot(rows_ref[...], w_ref[...]).astype(BF16)


def rows_mlp_kernel(steps, info, rows_ref, w1_ref, w3_ref, w2_ref, out_ref, act_ref):
    step = pl.program_id(0)

    @pl.when(step < steps)
    def _():
        wide = dot(rows_ref[...], w1_ref[...])
        cols = pl.ds(pl.multiple_of(step * ACT_COLS, ACT_COLS), ACT_COLS)
        act_ref[:, cols] = (wide * jax.nn.sigmoid(wide) * dot(rows_ref[...], w3_ref[...])).astype(BF16)

    @pl.when(step >= steps)
    def _():
        out_ref[...] = dot(act_ref[...], w2_ref[...]).astype(BF16)


def solution(mesh):
    dp_size, pp_size, tp_size = mesh.shape["dp"], mesh.shape["pp"], mesh.shape["tp"]
    grid = Mesh(mesh.devices.reshape(dp_size, pp_size, tp_size // 2, 2), ("dp", "pp", "x", "core"))
    down, up = [(0, 1)], [(1, 0)]

    def program(x_in, seq_len, norm_attn, w_qa, norm_q, w_qb, w_kva, norm_kv, w_kvb, w_o, norm_mlp, w_gate, w_up, w_down, norm_final):
        batch, seq, width = x_in.shape
        wq_down, wq_up, wkv_down, wkv_up = w_qa[0], w_qb[0], w_kva[0].T, w_kvb[0]
        wo_part, w1_part, w3_part, w2_part = w_o[0], w_gate[0], w_up[0], w_down[0]
        q_rank, kv_rank = norm_q.shape[1], norm_kv.shape[1]
        rope = wkv_down.shape[0] - kv_rank
        heads = (wq_up.shape[1] - wkv_up.shape[1] + wo_part.shape[0]) // rope
        v_head = wo_part.shape[0] // heads
        nope = wkv_up.shape[1] // heads - v_head
        hidden_cols = w1_part.shape[1]
        scale = SCALE_DEPTH / math.sqrt(w_qa.shape[0] * pp_size)
        stage, chip, core = (lax.axis_index(name).astype(jnp.int32) for name in ("pp", "x", "core"))
        active = (stage == 0).astype(jnp.int32)
        cos_t, sin_t = rope_tables(seq, rope)
        flat_x = x_in.reshape(batch * seq, width)
        half = seq // 2
        joined_cols = q_rank + kv_rank + 2 * rope
        msg_cols = kv_rank + 2 * rope
        chunks = batch // 2

        next_wkv = lax.ppermute(wkv_down, "pp", up)
        next_g_attn = lax.ppermute(norm_attn, "pp", up)
        next_g_kv = lax.ppermute(norm_kv, "pp", up)

        def down_proj(i, token):
            info = jnp.stack([active, 2 * i + core])
            steps = q_rank // DOWN_COLS
            return call(
                functools.partial(down_kernel, (q_rank, kv_rank, rope, steps)), (steps + 1,), info,
                [(flat_x, pl.BlockSpec((seq, width), lambda n, s: (s[1], 0))), (norm_attn, fixed(1, width)),
                 (wq_down, pl.BlockSpec((width, DOWN_COLS), lambda n, s: (0, jnp.minimum(n, steps - 1)))), (norm_q, fixed(1, q_rank)),
                 (wkv_down, ANY), (norm_kv, fixed(1, kv_rank)), (cos_t, fixed(seq, rope)), (sin_t, fixed(seq, rope)), (token, ANY)],
                [(((seq, joined_cols), BF16), fixed(seq, joined_cols)), (TOKEN, fixed(8, 128))],
                [pltpu.VMEM((seq, width), BF16), pltpu.VMEM((seq, q_rank), BF16), pltpu.VMEM(wkv_down.shape, BF16), pltpu.SemaphoreType.DMA],
                2 * seq * width * (q_rank + kv_rank + rope), 2 * (seq * width + width * joined_cols))

        def attention(i, own, other, token):
            lens = lax.slice_in_dim(seq_len, 2 * i, 2 * i + 2)
            info = jnp.stack([active, chip, jnp.where(core == 0, lens[0], lens[1]), jnp.where(core == 0, lens[1], lens[0])])
            steps, q_cols, kv_cols = 2 * heads // HEAD_BLOCK, HEAD_BLOCK * (nope + rope), HEAD_BLOCK * (nope + v_head)
            first = lambda n: jnp.minimum(n, steps - 1) // 2
            later = lambda n: jnp.maximum(n - steps, 0)
            out = (((seq, width), BF16), pl.BlockSpec((seq, OUT_COLS), lambda n, s: (0, later(n))))
            return call(
                functools.partial(attention_kernel, (q_rank, kv_rank, nope, rope, v_head, steps)), (steps + width // OUT_COLS,), info,
                [(own, ANY), (other, ANY), (wq_up, pl.BlockSpec((q_rank, q_cols), lambda n, s: (0, first(n)))),
                 (wkv_up, pl.BlockSpec((kv_rank, kv_cols), lambda n, s: (0, first(n)))),
                 (wo_part, pl.BlockSpec((heads * v_head, OUT_COLS), lambda n, s: (0, later(n)))),
                 (cos_t, fixed(seq, rope)), (sin_t, fixed(seq, rope)), (token, ANY)],
                [out, out, (TOKEN, fixed(8, 128))],
                [pltpu.VMEM((2, seq, joined_cols), BF16), pltpu.VMEM((2, seq, heads * v_head), BF16), pltpu.SemaphoreType.DMA((2,))],
                2 * 2 * seq * (q_rank * wq_up.shape[1] + kv_rank * wkv_up.shape[1] + heads * v_head * width + heads * 3 * v_head * seq),
                2 * (wq_up.size + wkv_up.size + wo_part.size + 2 * seq * width))

        def mlp(pieces, token):
            steps = hidden_cols // ACT_COLS
            first = lambda n: jnp.minimum(n, steps - 1)
            later = lambda n: jnp.maximum(n - steps, 0)
            out = (((seq, width), BF16), pl.BlockSpec((seq, OUT_COLS), lambda n, s: (0, later(n))))
            return call(
                functools.partial(mlp_kernel, steps), (steps + width // OUT_COLS,), jnp.stack([active, active]),
                [(m, ANY) for m in pieces] + [
                    (w1_part, pl.BlockSpec((width, ACT_COLS), lambda n, s: (0, first(n)))),
                    (w3_part, pl.BlockSpec((width, ACT_COLS), lambda n, s: (0, first(n)))),
                    (w2_part, pl.BlockSpec((hidden_cols, OUT_COLS), lambda n, s: (0, later(n)))), (token, ANY)],
                [out, out, (TOKEN, fixed(8, 128))],
                [pltpu.VMEM((2 * seq, width), BF16), pltpu.VMEM((2 * seq, hidden_cols), BF16), pltpu.SemaphoreType.DMA((4,))],
                2 * 2 * seq * width * hidden_cols * 3, 2 * (3 * width * hidden_cols + 4 * seq * width))

        ROW_STEP = 64
        low_rows = pl.BlockSpec((ROW_STEP, width), lambda n, s: (n, 0))
        high_rows = pl.BlockSpec((ROW_STEP, width), lambda n, s: (half // ROW_STEP + n, 0))

        def half_sum(near, other, token):
            return call(add_kernel, (half // ROW_STEP,), jnp.stack([active]),
                        [(near, high_rows), (other, high_rows), (token, ANY)],
                        [(((half, width), BF16), low_rows), (TOKEN, fixed(8, 128))], [], half * width, 6 * half * width)

        def residual(i, near, other, from_chip, token):
            info = jnp.stack([((2 * i + core) * 2 + chip) * (half // ROW_STEP)])
            return call(functools.partial(residual_kernel, scale), (half // ROW_STEP,), info,
                        [(flat_x, pl.BlockSpec((ROW_STEP, width), lambda n, s: (s[0] + n, 0))), (near, low_rows), (other, low_rows),
                         (from_chip, low_rows), (norm_mlp, fixed(1, width)), (token, ANY)],
                        [(((half, width), BF16), low_rows), (((half, width), BF16), low_rows), (TOKEN, fixed(8, 128))],
                        [], 8 * half * width, 12 * half * width)

        def next_latent(i, hidden, near, other, from_chip, token):
            mine = lax.slice_in_dim(seq_len, 2 * i, 2 * i + 2)
            info = jnp.stack([chip * (half // ROWS), chip, jnp.where(core == 0, mine[0], mine[1])])
            table = pl.BlockSpec((ROWS, rope), lambda n, s: (s[0] + n, 0))
            low = pl.BlockSpec((ROWS, width), lambda n, s: (n, 0))
            return call(functools.partial(next_kernel, scale, kv_rank), (half // ROWS,), info,
                        [(hidden, low), (near, low), (other, low), (from_chip, low), (next_g_attn, fixed(1, width)),
                         (next_wkv, fixed(*next_wkv.shape)), (next_g_kv, fixed(1, kv_rank)), (cos_t, table), (sin_t, table), (token, ANY)],
                        [(((half + 16, msg_cols), BF16), fixed(half + 16, msg_cols)), (TOKEN, fixed(8, 128))],
                        [pltpu.VMEM((8, width), F32)], 2 * half * width * (kv_rank + rope), 8 * half * width + 2 * next_wkv.size)

        def last_attention(lens, latent, rows):
            normed = rms_norm(rows, norm_attn[0])
            q_full = dot(rms_norm(dot(normed, wq_down).astype(BF16), norm_q[0]), wq_up).astype(BF16).reshape(2, heads, nope + rope)
            at = lens - 1
            q_full = jnp.concatenate([q_full[..., :nope], apply_rope(q_full[..., nope:], cos_t[at][:, None], sin_t[at][:, None])], axis=-1)
            q_full = jnp.broadcast_to(q_full[:, :, None], (2, heads, 16, nope + rope))
            info = jnp.concatenate([jnp.zeros((2,), jnp.int32), lens])
            blocks = heads // HEAD_BLOCK
            outs = call(functools.partial(last_kernel, (kv_rank, nope, rope, v_head)), (blocks,), info,
                        [(q_full, pl.BlockSpec((2, HEAD_BLOCK, 16, nope + rope), lambda n, s: (0, n, 0, 0))), (latent, fixed(2, seq, msg_cols)),
                         (wkv_up, pl.BlockSpec((kv_rank, HEAD_BLOCK * (nope + v_head)), lambda n, s: (0, n)))],
                        [(((2, 16, heads * v_head), BF16), pl.BlockSpec((2, 16, HEAD_BLOCK * v_head), lambda n, s: (0, 0, n)))],
                        [], 4 * seq * kv_rank * wkv_up.shape[1], 2 * wkv_up.size)[0]
            return outs[:, 0]

        def rows_matmul(rows, weight):
            count, depth = rows.shape
            return call(rows_kernel, (width // OUT_COLS,), jnp.stack([active]),
                        [(rows, fixed(count, depth)), (weight, pl.BlockSpec((depth, OUT_COLS), lambda n, s: (0, n)))],
                        [(((count, width), BF16), pl.BlockSpec((count, OUT_COLS), lambda n, s: (0, n)))],
                        [], 2 * count * weight.size, 2 * weight.size)[0]

        def rows_mlp(rows):
            count = rows.shape[0]
            steps = hidden_cols // ACT_COLS
            first = lambda n: jnp.minimum(n, steps - 1)
            later = lambda n: jnp.maximum(n - steps, 0)
            return call(functools.partial(rows_mlp_kernel, steps), (steps + width // OUT_COLS,), jnp.stack([active]),
                        [(rows, fixed(count, width)), (w1_part, pl.BlockSpec((width, ACT_COLS), lambda n, s: (0, first(n)))),
                         (w3_part, pl.BlockSpec((width, ACT_COLS), lambda n, s: (0, first(n)))),
                         (w2_part, pl.BlockSpec((hidden_cols, OUT_COLS), lambda n, s: (0, later(n))))],
                        [(((count, width), BF16), pl.BlockSpec((count, OUT_COLS), lambda n, s: (0, later(n))))],
                        [pltpu.VMEM((count, hidden_cols), BF16)], 6 * count * w1_part.size, 6 * w1_part.size)[0]

        token = jnp.zeros(*TOKEN)
        state = [dict() for _ in range(chunks)]

        def swap(value, axis, stage_of):
            return lax.ppermute(value, ("pp", axis), [(2 * stage_of, 2 * stage_of + 1), (2 * stage_of + 1, 2 * stage_of)])

        def run_down(i):
            nonlocal token
            own, token = down_proj(i, token)
            state[i].update(own=own, other=swap(own, "core", 0))

        def run_att(i):
            nonlocal token
            near, far, token = attention(i, state[i]["own"], state[i]["other"], token)
            state[i].update(near=near, from_core=swap(far, "core", 0))

        def run_suma(i):
            nonlocal token
            sent, token = half_sum(state[i]["near"], state[i]["from_core"], token)
            state[i].update(from_chip=swap(sent, "x", 0))

        run_summ = run_suma

        def run_res(i):
            nonlocal token
            s = state[i]
            s["hidden"], normed, token = residual(i, s["near"], s["from_core"], s["from_chip"], token)
            over = swap(normed, "x", 0)
            beside = swap(normed, "core", 0)
            s["pieces"] = (normed, over, beside, swap(over, "core", 0))

        def run_mlp(i):
            nonlocal token
            near, far, token = mlp(state[i]["pieces"], token)
            state[i].update(near=near, from_core=swap(far, "core", 0))

        def run_next(i):
            nonlocal token
            s = state[i]
            s["msg"], token = next_latent(i, s["hidden"], s["near"], s["from_core"], s["from_chip"], token)
            sent = lax.ppermute(s["msg"], "pp", down)
            over = swap(sent, "x", 1)
            s["msgs"] = (sent, over, swap(sent, "core", 1), swap(over, "core", 1))

        def in_order(flag, mine, other):
            return jnp.where(flag == 0, jnp.stack([mine, other]), jnp.stack([other, mine]))

        def second_stage(lens, msgs, own, other):
            pairs = [in_order(chip, msgs[0], msgs[1]), in_order(chip, msgs[2], msgs[3])]
            whole = in_order(core, *pairs)
            latent = whole[:, :, :half].reshape(2, seq, msg_cols)
            row = whole[:, :, half:].reshape(2, 2, 16 * msg_cols)[..., :width]
            row = row[:, 0] + row[:, 1]
            return last_attention(lens, latent, row), row, latent[..., :kv_rank], latent[..., kv_rank:kv_rank + rope]

        def first_stage(lens, msgs, own, other):
            cut = lambda first, last: in_order(core, own[:, first:last], other[:, first:last])
            return (jnp.zeros((2, heads * v_head), BF16), jnp.zeros((2, width), BF16),
                    cut(q_rank, q_rank + kv_rank), cut(q_rank + kv_rank, q_rank + kv_rank + rope))

        run = dict(down=run_down, att=run_att, suma=run_suma, res=run_res, mlp=run_mlp, summ=run_summ, next=run_next)
        for kind, i in ORDER:
            run[kind](i)
        ends = []
        for i, s in enumerate(state):
            lens = lax.slice_in_dim(seq_len, 2 * i, 2 * i + 2)
            ends.append(lax.cond(stage == pp_size - 1, second_stage, first_stage, lens, s["msgs"], s["own"], s["other"]))

        outs, hidden, cached, turned = (jnp.concatenate(group, axis=0) for group in zip(*ends))

        def add(base, part):
            for axis in ("core", "x"):
                part = (part.astype(F32) + swap(part, axis, 1).astype(F32)).astype(BF16)
            return (base.astype(F32) + scale * part.astype(F32)).astype(BF16)

        hidden = add(hidden, rows_matmul(outs, wo_part))
        hidden = add(hidden, rows_mlp(rms_norm(hidden, norm_mlp[0])))
        final = rms_norm(hidden, norm_final)
        final = jnp.where(stage == pp_size - 1, final, lax.ppermute(final, "pp", up))
        return cached[None], turned[None], final

    tp = ("x", "core")
    weight_specs = (P("pp", None), P("pp", None, None), P("pp", None), P("pp", None, tp), P("pp", None, None), P("pp", None),
                    P("pp", None, tp), P("pp", tp, None), P("pp", None), P("pp", None, tp), P("pp", None, tp), P("pp", tp, None))
    in_specs = (P("dp", None, None), P("dp")) + weight_specs + (P(None),)
    out_specs = (P("pp", "dp", None, None), P("pp", "dp", None, None), P("dp", None))
    return jax.shard_map(program, mesh=grid, in_specs=in_specs, out_specs=out_specs, check_vma=False)
```

```python
import functools
import math
import jax
import jax.numpy as jnp
import numpy as np
from jax import lax
from jax.experimental import pallas as pl
from jax.experimental.pallas import tpu as pltpu
from jax.sharding import Mesh, PartitionSpec as P

RMS_EPS = 1e-5
ROPE_BASE = 10000.0
SCALE_DEPTH = 1.4
BF16, F32 = jnp.bfloat16, jnp.float32
ROWS = 128
TALL = 256
WIDE = 256
SHORT = 32
HEAD_BLOCK = 4
OUT_COLS = 768
ACT_COLS = 256
DOWN_COLS = 256
VMEM_LIMIT = 60 * 2 ** 20


def dot(lhs, rhs):
    return jnp.dot(lhs, rhs, preferred_element_type=F32)


def dot_t(lhs, rhs):
    return lax.dot_general(lhs, rhs, (((1,), (1,)), ((), ())), preferred_element_type=F32)


def rms_wide(wide, gain):
    inv = lax.rsqrt(jnp.mean(wide * wide, axis=-1, keepdims=True) + RMS_EPS)
    return (wide * inv * gain).astype(BF16)


def rms_rows(x_ref, rows, count, gain_ref, out_ref):
    width, cols = x_ref.shape[1], 256
    squares = jnp.zeros((count, cols), F32)
    for first in range(0, width, cols):
        wide = x_ref[rows, first:first + cols].astype(F32)
        squares = squares + wide * wide
    inv = lax.rsqrt(jnp.sum(squares, axis=-1, keepdims=True) * (1.0 / width) + RMS_EPS)
    for first in range(0, width, cols):
        wide = x_ref[rows, first:first + cols].astype(F32)
        out_ref[rows, first:first + cols] = (wide * inv * gain_ref[:, first:first + cols].astype(F32)).astype(BF16)


def rms_norm(values_in, gain):
    return rms_wide(values_in.astype(F32), gain.astype(F32))


def rope_tables(seq, rope):
    inv_freq = (ROPE_BASE ** (-2.0 * np.arange(rope // 2) / rope)).astype(np.float32)
    angle = (np.arange(seq, dtype=np.float32)[:, None] * inv_freq[None, :]).astype(np.float64)
    cos_t, sin_t = np.cos(angle), np.sin(angle)
    tables = np.concatenate([cos_t, cos_t], axis=-1), np.concatenate([-sin_t, sin_t], axis=-1)
    return tuple(jnp.asarray(table.astype(np.float32)) for table in tables)


def apply_rope(values_in, cos_t, sin_t):
    half = values_in.shape[-1] // 2
    wide = values_in.astype(F32)
    swapped = jnp.concatenate([wide[..., half:], wide[..., :half]], axis=-1)
    return (wide * cos_t + swapped * sin_t).astype(BF16)


def call(kernel, grid, scalars, inputs, outputs, scratch, flops, moved):
    return pl.pallas_call(
        kernel,
        grid_spec=pltpu.PrefetchScalarGridSpec(
            num_scalar_prefetch=1, grid=grid,
            in_specs=[spec for _, spec in inputs], out_specs=[spec for _, spec in outputs], scratch_shapes=scratch),
        out_shape=[jax.ShapeDtypeStruct(shape, dtype) for (shape, dtype), _ in outputs],
        compiler_params=pltpu.CompilerParams(dimension_semantics=("arbitrary",) * len(grid), vmem_limit_bytes=VMEM_LIMIT),
        cost_estimate=pl.CostEstimate(flops=int(flops), transcendentals=0, bytes_accessed=int(moved)),
    )(scalars, *[array for array, _ in inputs])


ANY = pl.BlockSpec(memory_space=pl.ANY)
TOKEN = ((8, 128), F32)


def fixed(*shape):
    return pl.BlockSpec(shape, lambda *_: (0,) * len(shape))


NAMES = [
    "down_0", "down_1", "att_0", "down_2", "suma_0", "att_1",
    "down_3", "suma_1", "res_0", "att_2", "res_1", "att_3",
    "suma_2", "mlp_0", "res_2", "suma_3", "mlp_1", "summ_0",
    "res_3", "summ_1", "mlp_2", "next_0", "summ_2", "mlpx_3",
    "next_1", "next_2", "summ_3", "mlpo_3", "next_3",
]
ORDER = [(name[:-2], int(name[-1])) for name in NAMES]


def down_kernel(dims, info, x_ref, g_attn, wq_ref, g_q, wkv_hbm, g_kv, cos_ref, sin_ref, _, joined_ref, token_ref,
                u_ref, raw_ref, wkv_ref, sem):
    q_rank, kv_rank, rope, steps = dims
    step = pl.program_id(0)
    active = info[0] == 1
    copy = pltpu.make_async_copy(wkv_hbm, wkv_ref, sem)
    seq = x_ref.shape[0]

    @pl.when((step == 0) & active)
    def _():
        copy.start()
        for first in range(0, seq, ROWS):
            for inner in range(first, first + ROWS, 32):
                rms_rows(x_ref, pl.ds(inner, 32), 32, g_attn, u_ref)
            rows = pl.ds(first, ROWS)
            raw_ref[rows, :DOWN_COLS] = dot(u_ref[rows, :], wq_ref[...]).astype(BF16)

    @pl.when((step > 0) & (step < steps) & active)
    def _():
        cols = pl.ds(pl.multiple_of(step * DOWN_COLS, DOWN_COLS), DOWN_COLS)
        raw_ref[:, cols] = dot(u_ref[...], wq_ref[...]).astype(BF16)

    @pl.when((step == steps) & active)
    def _():
        copy.wait()
        low = dot_t(u_ref[...], wkv_ref[...]).astype(BF16)
        for first in range(0, seq, 32):
            rows = pl.ds(first, 32)
            joined_ref[rows, :q_rank] = rms_norm(raw_ref[rows, :], g_q[...])
            joined_ref[rows, q_rank:q_rank + kv_rank] = rms_norm(low[first:first + 32, :kv_rank], g_kv[...])
            joined_ref[rows, q_rank + kv_rank:] = jnp.concatenate(
                [apply_rope(low[first:first + 32, kv_rank:], cos_ref[rows, :], sin_ref[rows, :]), jnp.zeros((32, rope), BF16)], axis=-1)

    @pl.when(step == steps)
    def _():
        token_ref[...] = jnp.zeros_like(token_ref)


def attention_kernel(dims, info, own_hbm, other_hbm, wq_ref, wkv_ref, wo_ref, cos_ref, sin_ref, _, near_ref, far_ref, token_ref,
                     joined, q_ref, kv_ref, bias_ref, s_ref, p_ref, outs, sems):
    q_rank, kv_rank, nope, rope, v_head, steps = dims
    step = pl.program_id(0)
    active = info[0] == 1
    qk, seq = nope + rope, joined.shape[1]
    copies = [pltpu.make_async_copy(ref, joined.at[i], sems.at[i]) for i, ref in enumerate((own_hbm, other_hbm))]

    chip = info[1]
    half = seq // 2
    sides = near_ref, far_ref

    def projections(prompt):
        def piece(out_ref, w_ref, first, last, rows, cols):
            out_ref[prompt, rows, cols] = dot(joined[prompt, rows, first:last], w_ref[:, cols]).astype(BF16)

        for out_ref, w_ref, first, last in ((q_ref, wq_ref, 0, q_rank), (kv_ref, wkv_ref, q_rank, q_rank + kv_rank)):
            for col in range(0, out_ref.shape[2], WIDE):
                for row in range(0, seq, TALL):
                    yield functools.partial(piece, out_ref, w_ref, first, last, pl.ds(row, TALL), pl.ds(col, WIDE))

    def out_pieces(prompt):
        def piece(rows):
            sides[prompt][rows, :] = dot(outs[prompt, rows, :], wo_ref[...]).astype(BF16)

        return [functools.partial(piece, pl.ds(row, TALL)) for row in range(0, seq, TALL)]

    def attend(prompt, group, extra):
        length = info[2 + prompt]
        for first in range(0, seq, SHORT):
            limit = jnp.minimum(lax.broadcasted_iota(jnp.int32, (SHORT, 1), 0) + first, length - 1)
            bias_ref[pl.ds(first, SHORT), :] = jnp.where(lax.broadcasted_iota(jnp.int32, (SHORT, seq), 1) <= limit, 0.0, -1e30)

        def score(head, first):
            ends, rows, slot = first + TALL, pl.ds(first, TALL), head % 2
            pair, inner = head // 2 * 2 * qk, head % 2 * qk
            q_pair = q_ref[prompt, rows, pair:pair + 2 * qk]
            q_rope = apply_rope(q_pair[:, inner + nope:inner + qk], cos_ref[rows, :], sin_ref[rows, :])
            queries = jnp.concatenate([q_pair[:, inner:inner + nope], q_rope], axis=-1)
            base = head * (nope + v_head)
            keys = jnp.concatenate([kv_ref[prompt, :ends, base:base + nope], joined[prompt, :ends, q_rank + kv_rank:q_rank + kv_rank + rope]], axis=-1)
            scores = dot_t(queries, keys) * (qk ** -0.5 * math.log2(math.e))
            s_ref[slot, rows, :ends] = scores + bias_ref[rows, :ends]

        def value(head, first):
            ends, slot = first + TALL, head % 2
            base = head * (nope + v_head) + nope
            place = jnp.bitwise_xor(first // half, chip) * half + first % half
            cols = pl.ds(pl.multiple_of((group * HEAD_BLOCK + head) * v_head, v_head), v_head)
            outs[prompt, pl.ds(pl.multiple_of(place, TALL), TALL), cols] = dot(
                p_ref[slot, pl.ds(first, TALL), :ends], kv_ref[prompt, :ends, base:base + v_head]).astype(BF16)

        def softmax(head):
            slot = head % 2
            units = [(first, first // TALL * TALL + TALL) for first in range(0, seq, SHORT)]
            tops = {}
            for at in range(len(units) + 2):
                if at < len(units):
                    first, ends = units[at]
                    tops[at] = jnp.max(s_ref[slot, pl.ds(first, SHORT), :ends], axis=-1, keepdims=True)
                if 0 <= at - 1 < len(units):
                    first, ends = units[at - 1]
                    total = jnp.sum(jnp.exp2(s_ref[slot, pl.ds(first, SHORT), :ends] - tops[at - 1]), axis=-1, keepdims=True)
                    tops[at - 1] = tops[at - 1] + jnp.log2(total)
                if 0 <= at - 2:
                    first, ends = units[at - 2]
                    p_ref[slot, pl.ds(first, SHORT), :ends] = jnp.exp2(s_ref[slot, pl.ds(first, SHORT), :ends] - tops.pop(at - 2)).astype(BF16)
                yield

        rounds = HEAD_BLOCK + 2
        for head in range(rounds):
            work = [functools.partial(score, head, first) for first in range(0, seq, TALL)] if head < HEAD_BLOCK else []
            work += [functools.partial(value, head - 2, first) for first in range(0, seq, TALL)] if head >= 2 else []
            work += extra[len(extra) * head // rounds:len(extra) * (head + 1) // rounds]
            units = softmax(head - 1) if 1 <= head <= HEAD_BLOCK else iter(())
            for piece in work:
                piece()
                for _ in range(3):
                    next(units, None)
            for _ in units:
                pass

    @pl.when((step == 0) & active)
    def _():
        copies[0].start()
        copies[1].start()
        copies[0].wait()
        for piece in projections(0):
            piece()

    @pl.when((step == 1) & active)
    def _():
        copies[1].wait()

    for parity in range(2):
        @pl.when((step > 0) & (step < steps) & (step % 2 == parity) & active)
        def _():
            attend(1 - parity, (step - 1) // 2, list(projections(parity)))

    @pl.when((step == steps) & active)
    def _():
        attend(1, (step - 1) // 2, out_pieces(0))
        for piece in out_pieces(1):
            piece()

    @pl.when((step > steps) & active)
    def _():
        for piece in out_pieces(0) + out_pieces(1):
            piece()

    @pl.when(step == pl.num_programs(0) - 1)
    def _():
        token_ref[...] = jnp.zeros_like(token_ref)


def mlp_kernel(steps, count, info, *refs):
    pieces, (w1_ref, w3_ref, w2_ref, _, near_ref, far_ref, token_ref, rows_ref, act_ref, sems) = refs[:count], refs[count:]
    step = pl.program_id(0)
    active = info[0] == 1
    depth = pieces[0].shape[0]
    copies = [pltpu.make_async_copy(ref, rows_ref.at[pl.ds(i * depth, depth)], sems.at[i]) for i, ref in enumerate(pieces)]

    def gate(first_step):
        cols = pl.ds(pl.multiple_of(step * ACT_COLS, ACT_COLS), ACT_COLS)
        for i in range(count):
            if first_step:
                copies[i].wait()
            rows = pl.ds(i * depth, depth)
            wide = dot(rows_ref[rows, :], w1_ref[...])
            act_ref[rows, cols] = (wide * jax.nn.sigmoid(wide) * dot(rows_ref[rows, :], w3_ref[...])).astype(BF16)

    @pl.when((step == 0) & active)
    def _():
        for copy in copies:
            copy.start()
        gate(True)

    @pl.when((step > 0) & (step < steps) & active)
    def _():
        gate(False)

    @pl.when((step >= steps) & active)
    def _():
        for i in range(count):
            out_ref = near_ref if i < count // 2 else far_ref
            out_ref[pl.ds(i % (count // 2) * depth, depth), :] = dot(act_ref[pl.ds(i * depth, depth), :], w2_ref[...]).astype(BF16)

    @pl.when(step == pl.num_programs(0) - 1)
    def _():
        token_ref[...] = jnp.zeros_like(token_ref)


def add_kernel(info, a_ref, b_ref, _, out_ref, token_ref):
    out_ref[...] = (a_ref[...].astype(F32) + b_ref[...].astype(F32)).astype(BF16)
    token_ref[...] = jnp.zeros_like(token_ref)


def join_rows(scale, refs, gain_ref, h_ref, u_ref, rows):
    x_ref, near_ref, core_ref, chip_ref = refs
    count, width = x_ref.shape
    cols, block = 256, 32
    for first in range(0, count, block):
        at = pl.ds(first, block)
        squares = jnp.zeros((block, cols), F32)
        for col in range(0, width, cols):
            part = pl.ds(col, cols)
            both = (near_ref[at, part].astype(F32) + core_ref[at, part].astype(F32)).astype(BF16)
            branch = (both.astype(F32) + chip_ref[at, part].astype(F32)).astype(BF16)
            hidden = (x_ref[at, part].astype(F32) + scale * branch.astype(F32)).astype(BF16)
            h_ref[pl.ds(rows + first, block), part] = hidden
            squares = squares + hidden.astype(F32) * hidden.astype(F32)
        inv = lax.rsqrt(jnp.sum(squares, axis=-1, keepdims=True) * (1.0 / width) + RMS_EPS)
        for col in range(0, width, cols):
            part = pl.ds(col, cols)
            wide = h_ref[pl.ds(rows + first, block), part].astype(F32)
            u_ref[pl.ds(rows + first, block), part] = (wide * inv * gain_ref[:, part].astype(F32)).astype(BF16)


def residual_kernel(scale, info, x_ref, near_ref, core_ref, chip_ref, gain, _, h_ref, m_ref, token_ref):
    join_rows(scale, (x_ref, near_ref, core_ref, chip_ref), gain, h_ref, m_ref, 0)
    token_ref[...] = jnp.zeros_like(token_ref)


def next_kernel(scale, kv_rank, steps, info, x_ref, near_ref, core_ref, chip_ref, g_attn, wkv_hbm, g_kv, cos_ref, sin_ref, _,
                msg_ref, token_ref, h_ref, u_ref, wkv_ref, sem):
    step = pl.program_id(0)
    active = info[3] == 1
    total, width = h_ref.shape
    count = x_ref.shape[0]
    copy = pltpu.make_async_copy(wkv_hbm, wkv_ref, sem)

    @pl.when((step == 0) & active)
    def _():
        copy.start()

    @pl.when((step < steps) & active)
    def _():
        join_rows(scale, (x_ref, near_ref, core_ref, chip_ref), g_attn, h_ref, u_ref, pl.multiple_of(step * count, count))

    @pl.when((step == steps) & active)
    def _():
        copy.wait()
        low = dot_t(u_ref[...], wkv_ref[...]).astype(BF16)
        msg_ref[:total, :kv_rank] = rms_norm(low[:, :kv_rank], g_kv[...])
        turned = apply_rope(low[:, kv_rank:], cos_ref[...], sin_ref[...])
        msg_ref[:total, kv_rank:] = jnp.concatenate([turned, jnp.zeros_like(turned)], axis=-1)
        wanted = info[2] - 1 - info[1] * total
        block = jnp.clip(wanted // 16, 0, total // 16 - 1) * 16
        near = h_ref[pl.ds(pl.multiple_of(block, 16), 16), :].astype(F32)
        here = lax.broadcasted_iota(jnp.int32, (16, 1), 0) == wanted - block
        row = jnp.sum(jnp.where(here, near, 0.0), axis=0, keepdims=True)
        cols = msg_ref.shape[1]
        parts = []
        for first in range(0, width, cols):
            part = row[:, first:min(first + cols, width)]
            if part.shape[1] < cols:
                part = jnp.concatenate([part, jnp.zeros((1, cols - part.shape[1]), F32)], axis=-1)
            parts.append(part)
        parts.append(jnp.zeros((16 - len(parts), cols), F32))
        msg_ref[pl.ds(total, 16), :] = jnp.concatenate(parts, axis=0).astype(BF16)

    token_ref[...] = jnp.zeros_like(token_ref)


def last_kernel(dims, info, q_ref, c_ref, wkv_ref, out_ref):
    kv_rank, nope, rope, v_head = dims
    count = q_ref.shape[2]
    projected = [dot(c_ref[prompt, :, :kv_rank], wkv_ref[...]).astype(BF16) for prompt in range(2)]
    scores = []
    for prompt in range(2):
        k_rope = c_ref[prompt, :, kv_rank:kv_rank + rope]
        for head in range(HEAD_BLOCK):
            base = head * (nope + v_head)
            keys = jnp.concatenate([projected[prompt][:, base:base + nope], k_rope], axis=-1)
            found = dot_t(q_ref[prompt, head], keys) * (nope + rope) ** -0.5
            scores.append(jnp.where(lax.broadcasted_iota(jnp.int32, found.shape, 1) < info[2 + prompt], found, -1e30))
    scores = jnp.concatenate(scores, axis=0)
    grown = jnp.exp(scores - jnp.max(scores, axis=-1, keepdims=True))
    probs = grown * (1.0 / jnp.sum(grown, axis=-1, keepdims=True))
    for prompt in range(2):
        for head in range(HEAD_BLOCK):
            base = head * (nope + v_head) + nope
            at = (prompt * HEAD_BLOCK + head) * count
            out_ref[prompt, :, head * v_head:(head + 1) * v_head] = dot(
                probs[at:at + count].astype(BF16), projected[prompt][:, base:base + v_head]).astype(BF16)


def rows_kernel(info, rows_ref, w_ref, out_ref):
    out_ref[...] = dot(rows_ref[...], w_ref[...]).astype(BF16)


def rows_mlp_kernel(steps, act_cols, info, rows_ref, w1_ref, w3_ref, w2_ref, out_ref, act_ref):
    step = pl.program_id(0)

    @pl.when(step < steps)
    def _():
        wide = dot(rows_ref[...], w1_ref[...])
        cols = pl.ds(pl.multiple_of(step * act_cols, act_cols), act_cols)
        act_ref[:, cols] = (wide * jax.nn.sigmoid(wide) * dot(rows_ref[...], w3_ref[...])).astype(BF16)

    @pl.when(step >= steps)
    def _():
        out_ref[...] = dot(act_ref[...], w2_ref[...]).astype(BF16)


def solution(mesh):
    dp_size, pp_size, tp_size = mesh.shape["dp"], mesh.shape["pp"], mesh.shape["tp"]
    grid = Mesh(mesh.devices.reshape(dp_size, pp_size, tp_size // 2, 2), ("dp", "pp", "x", "core"))
    down, up = [(0, 1)], [(1, 0)]

    def program(x_in, seq_len, norm_attn, w_qa, norm_q, w_qb, w_kva, norm_kv, w_kvb, w_o, norm_mlp, w_gate, w_up, w_down, norm_final):
        batch, seq, width = x_in.shape
        wq_down, wq_up, wkv_down, wkv_up = w_qa[0], w_qb[0], w_kva[0].T, w_kvb[0]
        wo_part, w1_part, w3_part, w2_part = w_o[0], w_gate[0], w_up[0], w_down[0]
        q_rank, kv_rank = norm_q.shape[1], norm_kv.shape[1]
        rope = wkv_down.shape[0] - kv_rank
        heads = (wq_up.shape[1] - wkv_up.shape[1] + wo_part.shape[0]) // rope
        v_head = wo_part.shape[0] // heads
        nope = wkv_up.shape[1] // heads - v_head
        hidden_cols = w1_part.shape[1]
        scale = SCALE_DEPTH / math.sqrt(w_qa.shape[0] * pp_size)
        stage, chip, core = (lax.axis_index(name).astype(jnp.int32) for name in ("pp", "x", "core"))
        active = (stage == 0).astype(jnp.int32)
        cos_t, sin_t = rope_tables(seq, rope)
        flat_x = x_in.reshape(batch * seq, width)
        half = seq // 2
        joined_cols = q_rank + kv_rank + 2 * rope
        msg_cols = kv_rank + 2 * rope
        chunks = batch // 2

        next_wkv = lax.ppermute(wkv_down, "pp", up)
        next_g_attn = lax.ppermute(norm_attn, "pp", up)
        next_g_kv = lax.ppermute(norm_kv, "pp", up)

        def down_proj(i, token):
            info = jnp.stack([active, 2 * i + core])
            steps = q_rank // DOWN_COLS
            return call(
                functools.partial(down_kernel, (q_rank, kv_rank, rope, steps)), (steps + 1,), info,
                [(flat_x, pl.BlockSpec((seq, width), lambda n, s: (s[1], 0))), (norm_attn, fixed(1, width)),
                 (wq_down, pl.BlockSpec((width, DOWN_COLS), lambda n, s: (0, s[0] * jnp.minimum(n, steps - 1)))), (norm_q, fixed(1, q_rank)),
                 (wkv_down, ANY), (norm_kv, fixed(1, kv_rank)), (cos_t, fixed(seq, rope)), (sin_t, fixed(seq, rope)), (token, ANY)],
                [(((seq, joined_cols), BF16), fixed(seq, joined_cols)), (TOKEN, fixed(8, 128))],
                [pltpu.VMEM((seq, width), BF16), pltpu.VMEM((seq, q_rank), BF16), pltpu.VMEM(wkv_down.shape, BF16), pltpu.SemaphoreType.DMA],
                2 * seq * width * (q_rank + kv_rank + rope), 2 * (seq * width + width * joined_cols))

        def attention(i, own, other, token):
            lens = lax.slice_in_dim(seq_len, 2 * i, 2 * i + 2)
            info = jnp.stack([active, chip, jnp.where(core == 0, lens[0], lens[1]), jnp.where(core == 0, lens[1], lens[0])])
            steps, q_cols, kv_cols = 2 * heads // HEAD_BLOCK, HEAD_BLOCK * (nope + rope), HEAD_BLOCK * (nope + v_head)
            first = lambda n: jnp.minimum(n, steps - 1) // 2
            later = lambda n: jnp.maximum(n - steps, 0)
            out = (((seq, width), BF16), pl.BlockSpec((seq, OUT_COLS), lambda n, s: (0, later(n))))
            return call(
                functools.partial(attention_kernel, (q_rank, kv_rank, nope, rope, v_head, steps)), (steps + width // OUT_COLS,), info,
                [(own, ANY), (other, ANY), (wq_up, pl.BlockSpec((q_rank, q_cols), lambda n, s: (0, s[0] * first(n)))),
                 (wkv_up, pl.BlockSpec((kv_rank, kv_cols), lambda n, s: (0, s[0] * first(n)))),
                 (wo_part, pl.BlockSpec((heads * v_head, OUT_COLS), lambda n, s: (0, s[0] * later(n)))),
                 (cos_t, fixed(seq, rope)), (sin_t, fixed(seq, rope)), (token, ANY)],
                [out, out, (TOKEN, fixed(8, 128))],
                [pltpu.VMEM((2, seq, joined_cols), BF16), pltpu.VMEM((2, seq, q_cols), BF16), pltpu.VMEM((2, seq, kv_cols), BF16),
                 pltpu.VMEM((seq, seq), F32), pltpu.VMEM((2, seq, seq), F32), pltpu.VMEM((2, seq, seq), BF16), pltpu.VMEM((2, seq, heads * v_head), BF16),
                 pltpu.SemaphoreType.DMA((2,))],
                2 * 2 * seq * (q_rank * wq_up.shape[1] + kv_rank * wkv_up.shape[1] + heads * v_head * width + heads * 3 * v_head * seq),
                2 * (wq_up.size + wkv_up.size + wo_part.size + 2 * seq * width))

        def mlp(pieces, token):
            steps, count = hidden_cols // ACT_COLS, len(pieces)
            rows = count * half
            first = lambda n: jnp.minimum(n, steps - 1)
            later = lambda n: jnp.maximum(n - steps, 0)
            out = (((rows // 2, width), BF16), pl.BlockSpec((rows // 2, OUT_COLS), lambda n, s: (0, later(n))))
            return call(
                functools.partial(mlp_kernel, steps, count), (steps + width // OUT_COLS,), jnp.stack([active, active]),
                [(m, ANY) for m in pieces] + [
                    (w1_part, pl.BlockSpec((width, ACT_COLS), lambda n, s: (0, s[0] * first(n)))),
                    (w3_part, pl.BlockSpec((width, ACT_COLS), lambda n, s: (0, s[0] * first(n)))),
                    (w2_part, pl.BlockSpec((hidden_cols, OUT_COLS), lambda n, s: (0, s[0] * later(n)))), (token, ANY)],
                [out, out, (TOKEN, fixed(8, 128))],
                [pltpu.VMEM((rows, width), BF16), pltpu.VMEM((rows, hidden_cols), BF16), pltpu.SemaphoreType.DMA((count,))],
                2 * rows * width * hidden_cols * 3, 2 * (3 * width * hidden_cols + 2 * rows * width))

        ROW_STEP = 64
        low_rows = pl.BlockSpec((ROW_STEP, width), lambda n, s: (n, 0))
        high_rows = pl.BlockSpec((ROW_STEP, width), lambda n, s: (half // ROW_STEP + n, 0))

        def half_sum(near, other, token):
            spec = high_rows if near.shape[0] > half else low_rows
            return call(add_kernel, (half // ROW_STEP,), jnp.stack([active]),
                        [(near, spec), (other, spec), (token, ANY)],
                        [(((half, width), BF16), low_rows), (TOKEN, fixed(8, 128))], [], half * width, 6 * half * width)

        def residual(i, near, other, from_chip, token):
            info = jnp.stack([((2 * i + core) * 2 + chip) * (half // ROW_STEP)])
            return call(functools.partial(residual_kernel, scale), (half // ROW_STEP,), info,
                        [(flat_x, pl.BlockSpec((ROW_STEP, width), lambda n, s: (s[0] + n, 0))), (near, low_rows), (other, low_rows),
                         (from_chip, low_rows), (norm_mlp, fixed(1, width)), (token, ANY)],
                        [(((half, width), BF16), low_rows), (((half, width), BF16), low_rows), (TOKEN, fixed(8, 128))],
                        [], 8 * half * width, 12 * half * width)

        def next_latent(i, hidden, near, other, from_chip, token):
            mine = lax.slice_in_dim(seq_len, 2 * i, 2 * i + 2)
            info = jnp.stack([chip, chip, jnp.where(core == 0, mine[0], mine[1]), active])
            steps = half // ROW_STEP
            table = pl.BlockSpec((half, rope), lambda n, s: (s[0], 0))
            low = pl.BlockSpec((ROW_STEP, width), lambda n, s: (s[3] * jnp.minimum(n, steps - 1), 0))
            return call(functools.partial(next_kernel, scale, kv_rank, steps), (steps + 1,), info,
                        [(hidden, low), (near, low), (other, low), (from_chip, low), (next_g_attn, fixed(1, width)),
                         (next_wkv, ANY), (next_g_kv, fixed(1, kv_rank)), (cos_t, table), (sin_t, table), (token, ANY)],
                        [(((half + 16, msg_cols), BF16), fixed(half + 16, msg_cols)), (TOKEN, fixed(8, 128))],
                        [pltpu.VMEM((half, width), BF16), pltpu.VMEM((half, width), BF16), pltpu.VMEM(next_wkv.shape, BF16),
                         pltpu.SemaphoreType.DMA], 2 * half * width * (kv_rank + rope), 8 * half * width + 2 * next_wkv.size)

        def last_attention(lens, latent, rows):
            normed = rms_norm(rows, norm_attn[0])
            q_full = dot(rms_norm(dot(normed, wq_down).astype(BF16), norm_q[0]), wq_up).astype(BF16).reshape(2, heads, nope + rope)
            at = lens - 1
            q_full = jnp.concatenate([q_full[..., :nope], apply_rope(q_full[..., nope:], cos_t[at][:, None], sin_t[at][:, None])], axis=-1)
            q_full = jnp.broadcast_to(q_full[:, :, None], (2, heads, 8, nope + rope))
            info = jnp.concatenate([jnp.zeros((2,), jnp.int32), lens])
            blocks = heads // HEAD_BLOCK
            outs = call(functools.partial(last_kernel, (kv_rank, nope, rope, v_head)), (blocks,), info,
                        [(q_full, pl.BlockSpec((2, HEAD_BLOCK, 8, nope + rope), lambda n, s: (0, n, 0, 0))), (latent, fixed(2, seq, msg_cols)),
                         (wkv_up, pl.BlockSpec((kv_rank, HEAD_BLOCK * (nope + v_head)), lambda n, s: (0, n)))],
                        [(((2, 8, heads * v_head), BF16), pl.BlockSpec((2, 8, HEAD_BLOCK * v_head), lambda n, s: (0, 0, n)))],
                        [], 4 * seq * kv_rank * wkv_up.shape[1], 2 * wkv_up.size)[0]
            return outs[:, 0]

        def rows_matmul(rows, weight):
            count, depth = rows.shape
            cols = 2 * OUT_COLS
            return call(rows_kernel, (width // cols,), jnp.stack([active]),
                        [(rows, fixed(count, depth)), (weight, pl.BlockSpec((depth, cols), lambda n, s: (0, n)))],
                        [(((count, width), BF16), pl.BlockSpec((count, cols), lambda n, s: (0, n)))],
                        [], 2 * count * weight.size, 2 * weight.size)[0]

        def rows_mlp(rows):
            count, act_cols = rows.shape[0], 2 * ACT_COLS
            steps = hidden_cols // act_cols
            first = lambda n: jnp.minimum(n, steps - 1)
            later = lambda n: jnp.maximum(n - steps, 0)
            return call(functools.partial(rows_mlp_kernel, steps, act_cols), (steps + width // OUT_COLS,), jnp.stack([active]),
                        [(rows, fixed(count, width)), (w1_part, pl.BlockSpec((width, act_cols), lambda n, s: (0, first(n)))),
                         (w3_part, pl.BlockSpec((width, act_cols), lambda n, s: (0, first(n)))),
                         (w2_part, pl.BlockSpec((hidden_cols, OUT_COLS), lambda n, s: (0, later(n))))],
                        [(((count, width), BF16), pl.BlockSpec((count, OUT_COLS), lambda n, s: (0, later(n))))],
                        [pltpu.VMEM((count, hidden_cols), BF16)], 6 * count * w1_part.size, 6 * w1_part.size)[0]

        token = jnp.zeros(*TOKEN)
        state = [dict() for _ in range(chunks)]

        def swap(value, axis, stage_of):
            return lax.ppermute(value, ("pp", axis), [(2 * stage_of, 2 * stage_of + 1), (2 * stage_of + 1, 2 * stage_of)])

        def run_down(i):
            nonlocal token
            own, token = down_proj(i, token)
            state[i].update(own=own, other=swap(own, "core", 0))

        def run_att(i):
            nonlocal token
            near, far, token = attention(i, state[i]["own"], state[i]["other"], token)
            state[i].update(near=near, from_core=swap(far, "core", 0))

        def run_suma(i):
            nonlocal token
            sent, token = half_sum(state[i]["near"], state[i]["from_core"], token)
            state[i].update(from_chip=swap(sent, "x", 0))

        run_summ = run_suma

        def run_res(i):
            nonlocal token
            s = state[i]
            s["hidden"], normed, token = residual(i, s["near"], s["from_core"], s["from_chip"], token)
            over = swap(normed, "x", 0)
            beside = swap(normed, "core", 0)
            s["pieces"] = (normed, over, beside, swap(over, "core", 0))

        def run_mlp(i):
            nonlocal token
            near, far, token = mlp(state[i]["pieces"], token)
            state[i].update(near=near, from_core=swap(far, "core", 0))

        def run_mlpx(i):
            nonlocal token
            pieces = state[i]["pieces"]
            near, far, token = mlp((pieces[1], pieces[3]), token)
            state[i].update(near=near, from_core=swap(far, "core", 0))

        def run_mlpo(i):
            nonlocal token
            pieces = state[i]["pieces"]
            near, far, token = mlp((pieces[0], pieces[2]), token)
            state[i].update(near=near, from_core=swap(far, "core", 0))

        def run_next(i):
            nonlocal token
            s = state[i]
            s["msg"], token = next_latent(i, s["hidden"], s["near"], s["from_core"], s["from_chip"], token)
            sent = lax.ppermute(s["msg"], "pp", down)
            over = swap(sent, "x", 1)
            s["msgs"] = (sent, over, swap(sent, "core", 1), swap(over, "core", 1))

        def in_order(flag, mine, other):
            return jnp.where(flag == 0, jnp.stack([mine, other]), jnp.stack([other, mine]))

        def second_stage(lens, msgs, own, other):
            pairs = [in_order(chip, msgs[0], msgs[1]), in_order(chip, msgs[2], msgs[3])]
            whole = in_order(core, *pairs)
            latent = whole[:, :, :half].reshape(2, seq, msg_cols)
            row = whole[:, :, half:].reshape(2, 2, 16 * msg_cols)[..., :width]
            row = row[:, 0] + row[:, 1]
            return last_attention(lens, latent, row), row, latent[..., :kv_rank], latent[..., kv_rank:kv_rank + rope]

        def first_stage(lens, msgs, own, other):
            cut = lambda first, last: in_order(core, own[:, first:last], other[:, first:last])
            return (jnp.zeros((2, heads * v_head), BF16), jnp.zeros((2, width), BF16),
                    cut(q_rank, q_rank + kv_rank), cut(q_rank + kv_rank, q_rank + kv_rank + rope))

        run = dict(mlpx=run_mlpx, mlpo=run_mlpo, down=run_down, att=run_att, suma=run_suma, res=run_res, mlp=run_mlp, summ=run_summ, next=run_next)
        for kind, i in ORDER:
            run[kind](i)
        ends = []
        for i, s in enumerate(state):
            lens = lax.slice_in_dim(seq_len, 2 * i, 2 * i + 2)
            ends.append(lax.cond(stage == pp_size - 1, second_stage, first_stage, lens, s["msgs"], s["own"], s["other"]))

        outs, hidden, cached, turned = (jnp.concatenate(group, axis=0) for group in zip(*ends))

        def add(base, part):
            for axis in ("core", "x"):
                part = (part.astype(F32) + swap(part, axis, 1).astype(F32)).astype(BF16)
            return (base.astype(F32) + scale * part.astype(F32)).astype(BF16)

        hidden = add(hidden, rows_matmul(outs, wo_part))
        hidden = add(hidden, rows_mlp(rms_norm(hidden, norm_mlp[0])))
        final = rms_norm(hidden, norm_final)
        final = jnp.where(stage == pp_size - 1, final, lax.ppermute(final, "pp", up))
        return cached[None], turned[None], final

    tp = ("x", "core")
    weight_specs = (P("pp", None), P("pp", None, None), P("pp", None), P("pp", None, tp), P("pp", None, None), P("pp", None),
                    P("pp", None, tp), P("pp", tp, None), P("pp", None), P("pp", None, tp), P("pp", None, tp), P("pp", tp, None))
    in_specs = (P("dp", None, None), P("dp")) + weight_specs + (P(None),)
    out_specs = (P("pp", "dp", None, None), P("pp", "dp", None, None), P("dp", None))
    return jax.shard_map(program, mesh=grid, in_specs=in_specs, out_specs=out_specs, check_vma=False)
```
